32 devices in a mesh: tm: 2 (over x), src: 16 (over z, y, core).
Axes of the slice: x: 2, y: 2, z: 4, core: 2. Of those that a mesh axis runs over, the one named last changes fastest.
Arguments:
- design: float32 [16, 524288], P(None, ('tm', 'src')), may hold values from -2 to 2
- unit_index: int32 [524288], P(('tm', 'src')), may hold values from 0 to 255, as said below
- residual: float32 [524288], P(('tm', 'src')), may hold values from -6 to 6
- weight: float32 [524288], P(('tm', 'src')), may hold values from 0.25 to 4
- obs_count: int32 [32], P(('tm', 'src')), may hold values from 1 to 16384, as said below
- damping: float32 [256], P(('tm', 'src')), may hold values from 1 to 10
Outputs:
- solution: float32 [16, 256], P(None, ('tm', 'src'))
- misfit: float32 [], replicated
The draws below stay inside these ranges and needn't reach their ends.
Inputs may be any that keep to these rules, and one draw needn't show every extreme that they name: `unit_index`: an observation on a device of tm index g names a unit in [g * 128, (g + 1) * 128). `obs_count`: some device has all 16384 slots live.
All inputs are finite; a program needn't handle non-finite values.
Results may differ from the reference program's by a relative error of at most 0.0003.
Values sent between devices are 32-bit elements; how exact they have to be, the bound alone decides.
No kernel may reach another device: no remote copies, remote signals or barrier semaphores. Data moves between devices by JAX's collectives and lax.ppermute only.
A program may use at most 64 MiB of HBM per device.

```python
import math
import jax
import jax.numpy as jnp
from jax import lax

WIDTH = 16
OBS_DEV = 16384
UNITS_GRP = 128
UNITS = 256
OBS_ALL = 524288
N_SRC = 16
DEVICES = 32


def draw_unit_index(key, part):
    total = OBS_DEV * DEVICES
    group = jnp.arange(total, dtype=jnp.int32) // (OBS_DEV * N_SRC)
    picks = jax.random.randint(jax.random.fold_in(key, 11), (total,), 0, UNITS_GRP, dtype=jnp.int32)
    return picks + group * UNITS_GRP


def draw_obs_count(key, part):
    counts = jax.random.randint(jax.random.fold_in(key, 23), (DEVICES,), OBS_DEV // 8, OBS_DEV // 2 + 1, dtype=jnp.int32)
    return counts.at[0].set(OBS_DEV)


def block_scale(stream_key, extent, shards, least, top_value):
    def one(axis_at, blocks):
        steps = jax.random.uniform(jax.random.fold_in(jax.random.fold_in(stream_key, 6), axis_at), (blocks,), jnp.float32, least / len(shards), top_value / len(shards))
        return jnp.repeat(jnp.exp(steps), extent[axis_at] // blocks).reshape((-1,) + (1,) * (len(extent) - axis_at - 1))

    factor_of = one(*shards[0])
    for cut in shards[1:]:
        factor_of = factor_of * one(*cut)
    return factor_of


def bell_draw(own_key, dims, spread, bound, pieces=(), held_as=jnp.bfloat16):
    entries = spread * jax.random.normal(own_key, dims, jnp.float32)
    if pieces:
        entries = entries * block_scale(own_key, dims, pieces, -0.22, 0.18)
    return jnp.clip(entries, -bound, bound).astype(held_as)


def setup_inputs(seed: int = 0) -> dict:
    key_of = jax.random.split(jax.random.key(seed), 7)
    design = bell_draw(key_of[0], (WIDTH, OBS_ALL), 0.25, 2.0, ((1, 32),), jnp.float32)
    unit_index = draw_unit_index(jax.random.fold_in(key_of[6], 71), 0)
    residual = bell_draw(key_of[2], (OBS_ALL,), 1.0, 6.0, ((0, 32),), jnp.float32)
    weight = jnp.clip(jnp.exp(math.log(4.0) - 2.7725887 * jax.random.uniform(key_of[3], (OBS_ALL,), jnp.float32) ** block_scale(key_of[3], (OBS_ALL,), ((0, 32),), -0.2, 0.2)), 0.25, 4.0)
    obs_count = draw_obs_count(jax.random.fold_in(key_of[6], 71), 0)
    damping = jnp.clip(jnp.exp(math.log(10.0) - 2.3025851 * jax.random.uniform(key_of[5], (UNITS,), jnp.float32) ** block_scale(key_of[5], (UNITS,), ((0, 32),), -0.2, 0.2)), 1.0, 10.0)
    return dict(design=design, unit_index=unit_index, residual=residual, weight=weight, obs_count=obs_count, damping=damping)


def block_solve(normal, rhs, damping):
    lower = {}
    for j in range(16):
        running = normal[j * 16 + j] + damping
        for k in range(j):
            running = running - lower[j, k] * lower[j, k]
        diag_term = jnp.sqrt(running)
        lower[j, j] = diag_term
        for i in range(j + 1, 16):
            running = normal[i * 16 + j]
            for k in range(j):
                running = running - lower[i, k] * lower[j, k]
            lower[i, j] = running / diag_term
    forward = []
    for i in range(16):
        running = rhs[i]
        for k in range(i):
            running = running - lower[i, k] * forward[k]
        forward.append(running / lower[i, i])
    backward = [None] * 16
    for i in range(15, -1, -1):
        running = forward[i]
        for k in range(i + 1, 16):
            running = running - lower[k, i] * backward[k]
        backward[i] = running / lower[i, i]
    return jnp.stack(backward)

def reference(design, unit_index, residual, weight, obs_count, damping):
    units = damping.shape[0]
    blocks = obs_count.shape[0]
    design_blocks = design.reshape(16, blocks, -1).transpose(1, 0, 2)
    unit_blocks = unit_index.reshape(blocks, -1)
    resid_blocks = residual.reshape(blocks, -1)
    weight_blocks = weight.reshape(blocks, -1)
    slots = design_blocks.shape[2]

    def accumulate(carry, item):
        normal_sum, rhs_sum, weight_sum = carry
        rows, units_of, resid, weights, count = item
        weights_on = jnp.where(jnp.arange(slots, dtype=jnp.int32) < count, weights, jnp.zeros_like(weights))
        outer = (rows[:, None, :] * rows[None, :, :]).reshape(256, slots) * weights_on
        normal_sum = normal_sum.at[:, units_of].add(outer)
        rhs_sum = rhs_sum.at[:, units_of].add(rows * (weights_on * resid))
        return ((normal_sum, rhs_sum, weight_sum + jnp.sum(weights_on)), None)
    start = (jnp.zeros((256, units), jnp.float32), jnp.zeros((16, units), jnp.float32), jnp.zeros((), jnp.float32))
    (normal, rhs, weight_total), _ = lax.scan(accumulate, start, (design_blocks, unit_blocks, resid_blocks, weight_blocks, obs_count))
    solution = block_solve(normal, rhs, damping)

    def squares(carry, item):
        rows, units_of, resid, weights, count = item
        weights_on = jnp.where(jnp.arange(slots, dtype=jnp.int32) < count, weights, jnp.zeros_like(weights))
        fitted = lax.optimization_barrier(jnp.sum(rows * solution[:, units_of], axis=0))
        after = resid - fitted
        return (carry + jnp.sum(weights_on * after * after), None)
    chi_total, _ = lax.scan(squares, jnp.zeros((), jnp.float32), (design_blocks, unit_blocks, resid_blocks, weight_blocks, obs_count))
    return (solution, chi_total / weight_total)
```

```python
import jax
import jax.numpy as jnp
from jax import lax
from jax.experimental import pallas as pl
from jax.experimental.pallas import tpu as pltpu
from jax.sharding import PartitionSpec as P

HIGHER = 5
CROSS = 8
ROWS = 160
ROW_WEIGHT, ROW_BEFORE, ROW_DAMPING = 36, 37, 38
CHUNK = 4096
PIECE = 1024


def row_of(i, j):
    if i < 8 or j >= 8:
        base = 0 if i < 8 else 40
        a, b = i % 8, j % 8
        s = a - b
        return base + (s * 8 + b if s <= 4 else (8 - s) * 8 + a)
    return 80 + ((i - 8 - j) % 8) * 8 + j


def accumulate_kernel(count_ref, design_ref, unit_ref, resid_ref, weight_ref, damping_ref, keep_ref, send_ref, acc_ref, side_ref):
    step = pl.program_id(0)
    chunk = design_ref.shape[1]
    units = acc_ref.shape[1]
    piece = min(PIECE, chunk)
    src = lax.axis_index("src")
    first_unit = lax.axis_index("tm") * units
    count = count_ref[0]

    @pl.when(step == 0)
    def _():
        acc_ref[...] = jnp.zeros_like(acc_ref)
        side_ref[...] = jnp.zeros_like(side_ref)

    unit_rows = lax.broadcasted_iota(jnp.int32, (units, piece), 0)
    slot = lax.broadcasted_iota(jnp.int32, (1, piece), 1) + step * chunk
    total = jnp.zeros((2 * ROWS, units), jnp.float32)
    weight_sum = jnp.zeros((1, 128), jnp.float32)
    before_sum = jnp.zeros((1, 128), jnp.float32)
    for begin in range(0, chunk, piece):
        at = pl.ds(begin, piece)
        rows = design_ref[:, at]
        resid = resid_ref[:, at]
        weight = jnp.where(slot + begin < count, weight_ref[:, at], 0.0)
        first, second = rows[:8], rows[8:]
        wfirst, wsecond = first * weight, second * weight
        groups = [wfirst * (pltpu.roll(first, 8 - s, 0) if s else first) for s in range(HIGHER)]
        turned = [pltpu.roll(second, 8 - s, 0) if s else second for s in range(CROSS)]
        groups += [wsecond * turned[s] for s in range(HIGHER)]
        groups += [wfirst * turned[s] for s in range(CROSS)]
        groups += [wfirst * resid, wsecond * resid]
        high, low = [], []
        for a, b in zip(groups[::2], groups[1::2]):
            both = jnp.concatenate([a, b], axis=0)
            top = both.astype(jnp.bfloat16)
            high.append(top)
            low.append((both - top.astype(jnp.float32)).astype(jnp.bfloat16))
        stacked = jnp.concatenate(high + low, axis=0)
        local = unit_ref[:, at] - first_unit
        one_hot = jnp.where(unit_rows == local, 1.0, 0.0).astype(jnp.bfloat16)
        total = total + lax.dot_general(stacked, one_hot, (((1,), (1,)), ((), ())), preferred_element_type=jnp.float32)
        before = weight * resid * resid
        for k in range(0, piece, 128):
            weight_sum = weight_sum + weight[:, k:k + 128]
            before_sum = before_sum + before[:, k:k + 128]
    acc_ref[...] += total[:ROWS] + total[ROWS:]
    side_ref[0:1] += weight_sum
    side_ref[1:2] += before_sum

    @pl.when(step == pl.num_programs(0) - 1)
    def _():
        acc_ref[ROW_WEIGHT:ROW_DAMPING + 1, :] = jnp.zeros((3, units), jnp.float32)
        acc_ref[ROW_WEIGHT:ROW_BEFORE + 1, 0:128] = side_ref[0:2]
        own = damping_ref.shape[1]
        padded = jnp.concatenate([damping_ref[...], jnp.zeros((1, units - own), jnp.float32)], axis=1)
        placed = pltpu.roll(jnp.broadcast_to(padded, (8, units)), src * own, 1)
        acc_ref[ROW_DAMPING:ROW_DAMPING + 1, :] = placed[0:1]
        half = ROWS // 2
        bit = src % 2
        keep_ref[...] = acc_ref[pl.ds(pl.multiple_of(bit * half, 8), half), :]
        send_ref[...] = acc_ref[pl.ds(pl.multiple_of((1 - bit) * half, 8), half), :]


def solve_kernel(mine_ref, other_ref, solution_ref, stats_ref, full_ref, column_ref):
    units = mine_ref.shape[1]
    own = solution_ref.shape[1]
    src = lax.axis_index("src")
    half = ROWS // 2
    bit = src % 2
    full_ref[pl.ds(pl.multiple_of(bit * half, 8), half), :] = mine_ref[...]
    full_ref[pl.ds(pl.multiple_of((1 - bit) * half, 8), half), :] = other_ref[...]
    column_ref[...] = jnp.zeros_like(column_ref)
    for j in range(16):
        for i in range(j, 16):
            r = row_of(i, j)
            column_ref[j * 24 + i:j * 24 + i + 1, :] = full_ref[r:r + 1, :]
        column_ref[j * 24 + 16:j * 24 + 17, :] = full_ref[144 + j:145 + j, :]
    damping = full_ref[ROW_DAMPING:ROW_DAMPING + 1, :]
    upper = [column_ref[j * 24:j * 24 + 8, :] for j in range(8)]
    lower = [column_ref[j * 24 + 8:j * 24 + 24, :] for j in range(16)]

    def entry(top, bottom, i):
        return top[i:i + 1] if i < 8 else bottom[i - 8:i - 7]

    inverse, forward = [], []
    for j in range(16):
        inv = lax.rsqrt(entry(upper[j] if j < 8 else None, lower[j], j) + damping)
        inverse.append(inv)
        if j < 8:
            upper[j] = upper[j] * inv
        lower[j] = lower[j] * inv
        forward.append(lower[j][8:9])
        for k in range(j + 1, 16):
            factor = entry(upper[j] if j < 8 else None, lower[j], k)
            lower[k] = lower[k] - lower[j] * factor
            if k < 8:
                upper[k] = upper[k] - upper[j] * factor
    sub = lax.broadcasted_iota(jnp.int32, (8, units), 0)
    low_x = jnp.zeros((8, units), jnp.float32)
    high_x = jnp.zeros((8, units), jnp.float32)
    for i in range(15, -1, -1):
        part = lower[i][:8] * high_x
        if i < 8:
            part = part + upper[i] * low_x
        x = (forward[i] - jnp.sum(part, axis=0, keepdims=True)) * inverse[i]
        if i < 8:
            low_x = jnp.where(sub == i, x, low_x)
        else:
            high_x = jnp.where(sub == i - 8, x, high_x)
    squares = damping * jnp.sum(low_x * low_x + high_x * high_x, axis=0, keepdims=True)
    for y in forward:
        squares = squares + y * y
    chi = jnp.sum(full_ref[ROW_BEFORE:ROW_BEFORE + 1, :] - squares, axis=1, keepdims=True)
    weight = jnp.sum(full_ref[ROW_WEIGHT:ROW_WEIGHT + 1, :], axis=1, keepdims=True)
    stats_ref[...] = jnp.where(lax.broadcasted_iota(jnp.int32, (8, 128), 0) == 0, chi, weight)
    shift = (units - src * own) % units
    solution_ref[0:8, :] = pltpu.roll(low_x, shift, 1)[:, :own]
    solution_ref[8:16, :] = pltpu.roll(high_x, shift, 1)[:, :own]


def swap(x, axis, mask):
    size = lax.axis_size(axis)
    return lax.ppermute(x, axis, [(k, k ^ mask) for k in range(size)])


def masks_of(size):
    masks = []
    b = 1
    while (1 << b) < size:
        masks.append((1 << b) if b < 3 else (1 << b) | (1 << (b - 1)))
        b += 1
    return masks


def on_device(design, unit_index, residual, weight, obs_count, damping):
    n_source = lax.axis_size("src")
    own_units = damping.shape[0]
    units = own_units * n_source
    slots = design.shape[1]
    chunk = min(CHUNK, slots)
    half = ROWS // 2
    line = lambda: pl.BlockSpec((1, chunk), lambda s: (0, s))
    keep, send = pl.pallas_call(
        accumulate_kernel,
        grid=(slots // chunk,),
        in_specs=[
            pl.BlockSpec(memory_space=pltpu.SMEM),
            pl.BlockSpec((16, chunk), lambda s: (0, s)),
            line(), line(), line(),
            pl.BlockSpec((1, own_units), lambda s: (0, 0)),
        ],
        out_specs=[pl.BlockSpec((half, units), lambda s: (0, 0))] * 2,
        out_shape=[jax.ShapeDtypeStruct((half, units), jnp.float32)] * 2,
        scratch_shapes=[pltpu.VMEM((ROWS, units), jnp.float32), pltpu.VMEM((8, 128), jnp.float32)],
        compiler_params=pltpu.CompilerParams(dimension_semantics=("arbitrary",)),
        name="accumulate",
    )(obs_count, design, unit_index.reshape(1, slots), residual.reshape(1, slots), weight.reshape(1, slots), damping.reshape(1, own_units))
    mine = keep + swap(send, "src", 1)
    for mask in masks_of(n_source):
        mine = mine + swap(mine, "src", mask)
    other = swap(mine, "src", 1)
    solution_own, stats = pl.pallas_call(
        solve_kernel,
        out_shape=[jax.ShapeDtypeStruct((16, own_units), jnp.float32), jax.ShapeDtypeStruct((8, 128), jnp.float32)],
        scratch_shapes=[pltpu.VMEM((ROWS, units), jnp.float32), pltpu.VMEM((16 * 24, units), jnp.float32)],
        name="solve",
    )(mine, other)
    n_time = lax.axis_size("tm")
    mask = 1
    while mask < n_time:
        stats = stats + swap(stats, "tm", mask)
        mask *= 2
    return (solution_own, stats[0, 0] / stats[1, 0])


def solution(mesh):
    placed = (
        P(None, ("tm", "src")),
        P(("tm", "src")),
        P(("tm", "src")),
        P(("tm", "src")),
        P(("tm", "src")),
        P(("tm", "src")),
    )
    return jax.shard_map(
        on_device,
        mesh=mesh,
        in_specs=placed,
        out_specs=(P(None, ("tm", "src")), P()),
        check_vma=False,
    )
```

```python
import jax
import jax.numpy as jnp
from jax import lax
from jax.experimental import pallas as pl
from jax.experimental.pallas import tpu as pltpu
from jax.sharding import PartitionSpec as P

HIGHER = 5
CROSS = 8
ROWS = 160
ROW_WEIGHT, ROW_BEFORE, ROW_DAMPING = 36, 37, 38
CHUNK = 8192
PIECE = 2048


def row_of(i, j):
    if i < 8 or j >= 8:
        base = 0 if i < 8 else 40
        a, b = i % 8, j % 8
        s = a - b
        return base + (s * 8 + b if s <= 4 else (8 - s) * 8 + a)
    return 80 + ((i - 8 - j) % 8) * 8 + j


def accumulate_kernel(count_ref, design_ref, unit_ref, resid_ref, weight_ref, damping_ref, keep_ref, send_ref, acc_ref, side_ref):
    step = pl.program_id(0)
    chunk = design_ref.shape[1]
    units = acc_ref.shape[1]
    piece = min(PIECE, chunk)
    src = lax.axis_index("src")
    first_unit = lax.axis_index("tm") * units
    count = count_ref[...]

    @pl.when(step == 0)
    def _():
        acc_ref[...] = jnp.zeros_like(acc_ref)
        side_ref[...] = jnp.zeros_like(side_ref)

    unit_rows = lax.broadcasted_iota(jnp.int32, (units, piece), 0)
    slot = lax.broadcasted_iota(jnp.int32, (1, piece), 1) + step * chunk
    total = jnp.zeros((2 * ROWS, units), jnp.float32)
    weight_sum = jnp.zeros((1, 128), jnp.float32)
    before_sum = jnp.zeros((1, 128), jnp.float32)
    for begin in range(0, chunk, piece):
        at = pl.ds(begin, piece)
        rows = design_ref[:, at]
        resid = resid_ref[:, at]
        weight = jnp.where(slot + begin < count, weight_ref[:, at], 0.0)
        first, second = rows[:8], rows[8:]
        wfirst, wsecond = first * weight, second * weight
        groups = [wfirst * (pltpu.roll(first, 8 - s, 0) if s else first) for s in range(HIGHER)]
        turned = [pltpu.roll(second, 8 - s, 0) if s else second for s in range(CROSS)]
        groups += [wsecond * turned[s] for s in range(HIGHER)]
        groups += [wfirst * turned[s] for s in range(CROSS)]
        groups += [wfirst * resid, wsecond * resid]
        high, low = [], []
        for a, b in zip(groups[::2], groups[1::2]):
            both = jnp.concatenate([a, b], axis=0)
            top = both.astype(jnp.bfloat16)
            high.append(top)
            low.append((both - top.astype(jnp.float32)).astype(jnp.bfloat16))
        stacked = jnp.concatenate(high + low, axis=0)
        local = unit_ref[:, at] - first_unit
        one_hot = jnp.where(unit_rows == local, 1.0, 0.0).astype(jnp.bfloat16)
        total = total + lax.dot_general(stacked, one_hot, (((1,), (1,)), ((), ())), preferred_element_type=jnp.float32)
        before = weight * resid * resid
        for k in range(0, piece, 128):
            weight_sum = weight_sum + weight[:, k:k + 128]
            before_sum = before_sum + before[:, k:k + 128]
    acc_ref[...] += total[:ROWS] + total[ROWS:]
    side_ref[0:1] += weight_sum
    side_ref[1:2] += before_sum

    @pl.when(step == pl.num_programs(0) - 1)
    def _():
        acc_ref[ROW_WEIGHT:ROW_DAMPING + 1, :] = jnp.zeros((3, units), jnp.float32)
        acc_ref[ROW_WEIGHT:ROW_BEFORE + 1, 0:128] = side_ref[0:2]
        own = damping_ref.shape[1]
        padded = jnp.concatenate([damping_ref[...], jnp.zeros((1, units - own), jnp.float32)], axis=1)
        placed = pltpu.roll(jnp.broadcast_to(padded, (8, units)), src * own, 1)
        acc_ref[ROW_DAMPING:ROW_DAMPING + 1, :] = placed[0:1]
        half = ROWS // 2
        bit = src % 2
        keep_ref[...] = acc_ref[pl.ds(pl.multiple_of(bit * half, 8), half), :]
        send_ref[...] = acc_ref[pl.ds(pl.multiple_of((1 - bit) * half, 8), half), :]


def solve_kernel(mine_ref, other_ref, solution_ref, stats_ref, full_ref, column_ref):
    units = mine_ref.shape[1]
    own = solution_ref.shape[0]
    src = lax.axis_index("src")
    half = ROWS // 2
    bit = src % 2
    full_ref[pl.ds(pl.multiple_of(bit * half, 8), half), :] = mine_ref[...]
    full_ref[pl.ds(pl.multiple_of((1 - bit) * half, 8), half), :] = other_ref[...]
    column_ref[...] = jnp.zeros_like(column_ref)
    for j in range(16):
        for i in range(j, 16):
            r = row_of(i, j)
            column_ref[j * 24 + i:j * 24 + i + 1, :] = full_ref[r:r + 1, :]
        column_ref[j * 24 + 16:j * 24 + 17, :] = full_ref[144 + j:145 + j, :]
    damping = full_ref[ROW_DAMPING:ROW_DAMPING + 1, :]
    upper = [column_ref[j * 24:j * 24 + 8, :] for j in range(8)]
    lower = [column_ref[j * 24 + 8:j * 24 + 24, :] for j in range(16)]

    def entry(top, bottom, i):
        return top[i:i + 1] if i < 8 else bottom[i - 8:i - 7]

    inverse, forward = [], []
    for j in range(16):
        inv = lax.rsqrt(entry(upper[j] if j < 8 else None, lower[j], j) + damping)
        inverse.append(inv)
        if j < 8:
            upper[j] = upper[j] * inv
        lower[j] = lower[j] * inv
        forward.append(lower[j][8:9])
        for k in range(j + 1, 16):
            factor = entry(upper[j] if j < 8 else None, lower[j], k)
            lower[k] = lower[k] - lower[j] * factor
            if k < 8:
                upper[k] = upper[k] - upper[j] * factor
    sub = lax.broadcasted_iota(jnp.int32, (8, units), 0)
    low_x = jnp.zeros((8, units), jnp.float32)
    high_x = jnp.zeros((8, units), jnp.float32)
    for i in range(15, -1, -1):
        part = lower[i][:8] * high_x
        if i < 8:
            part = part + upper[i] * low_x
        x = (forward[i] - jnp.sum(part, axis=0, keepdims=True)) * inverse[i]
        if i < 8:
            low_x = jnp.where(sub == i, x, low_x)
        else:
            high_x = jnp.where(sub == i - 8, x, high_x)
    squares = damping * jnp.sum(low_x * low_x + high_x * high_x, axis=0, keepdims=True)
    for y in forward:
        squares = squares + y * y
    chi = jnp.sum(full_ref[ROW_BEFORE:ROW_BEFORE + 1, :] - squares, axis=1, keepdims=True)
    weight = jnp.sum(full_ref[ROW_WEIGHT:ROW_WEIGHT + 1, :], axis=1, keepdims=True)
    stats_ref[...] = jnp.where(lax.broadcasted_iota(jnp.int32, (8, 128), 0) == 0, chi, weight)
    shift = (units - src * own) % units
    turned = pltpu.roll(jnp.concatenate([low_x, high_x], axis=0), shift, 1)
    solution_ref[...] = turned[:, :128].T[:own]


def quotient_kernel(own_ref, other_ref, out_ref):
    total = own_ref[...] + other_ref[...]
    out_ref[...] = total[0:1, 0:1] / total[1:2, 0:1]


def in_vmem(x):
    return pltpu.with_memory_space_constraint(x, pltpu.VMEM)


def swap(x, axis, mask):
    size = lax.axis_size(axis)
    return lax.ppermute(x, axis, [(k, k ^ mask) for k in range(size)])


def masks_of(size):
    masks = []
    b = 1
    while (1 << b) < size:
        masks.append(1 << b)
        b += 1
    return masks


def on_device(design, unit_index, residual, weight, obs_count, damping):
    n_source = lax.axis_size("src")
    own_units = damping.shape[0]
    units = own_units * n_source
    slots = design.shape[1]
    chunk = min(CHUNK, slots)
    half = ROWS // 2
    line = lambda: pl.BlockSpec((1, chunk), lambda s: (0, s))
    keep, send = pl.pallas_call(
        accumulate_kernel,
        grid=(slots // chunk,),
        in_specs=[
            pl.BlockSpec((1, 1), lambda s: (0, 0)),
            pl.BlockSpec((16, chunk), lambda s: (0, s)),
            line(), line(), line(),
            pl.BlockSpec((1, own_units), lambda s: (0, 0)),
        ],
        out_specs=[pl.BlockSpec(memory_space=pltpu.VMEM)] * 2,
        out_shape=[pltpu.VMEM((half, units), jnp.float32)] * 2,
        scratch_shapes=[pltpu.VMEM((ROWS, units), jnp.float32), pltpu.VMEM((8, 128), jnp.float32)],
        compiler_params=pltpu.CompilerParams(dimension_semantics=("arbitrary",)),
        name="accumulate",
    )(obs_count.reshape(1, 1), design, unit_index.reshape(1, slots), residual.reshape(1, slots), weight.reshape(1, slots), damping.reshape(1, own_units))
    mine = keep + swap(send, "src", 1)
    for mask in masks_of(n_source):
        mine = mine + swap(mine, "src", mask)
    other = swap(mine, "src", 1)
    solution_own, stats = pl.pallas_call(
        solve_kernel,
        in_specs=[pl.BlockSpec(memory_space=pltpu.VMEM)] * 2,
        out_specs=[pl.BlockSpec(memory_space=pltpu.VMEM)] * 2,
        out_shape=[jax.ShapeDtypeStruct((own_units, 16), jnp.float32), pltpu.VMEM((8, 128), jnp.float32)],
        scratch_shapes=[pltpu.VMEM((ROWS, units), jnp.float32), pltpu.VMEM((16 * 24, units), jnp.float32)],
        name="solve",
    )(in_vmem(mine), in_vmem(other))
    n_time = lax.axis_size("tm")
    mask = 1
    while 2 * mask < n_time:
        stats = stats + swap(stats, "tm", mask)
        mask *= 2
    last = swap(stats, "tm", mask) if n_time > 1 else jnp.zeros_like(stats)
    misfit = pl.pallas_call(
        quotient_kernel,
        in_specs=[pl.BlockSpec(memory_space=pltpu.VMEM)] * 2,
        out_shape=jax.ShapeDtypeStruct((1, 1), jnp.float32),
        name="quotient",
    )(in_vmem(stats), in_vmem(last))
    return (solution_own.T, misfit.reshape(()))


def solution(mesh):
    placed = (
        P(None, ("tm", "src")),
        P(("tm", "src")),
        P(("tm", "src")),
        P(("tm", "src")),
        P(("tm", "src")),
        P(("tm", "src")),
    )
    return jax.shard_map(
        on_device,
        mesh=mesh,
        in_specs=placed,
        out_specs=(P(None, ("tm", "src")), P()),
        check_vma=False,
    )
```

```python
import jax
import jax.numpy as jnp
from jax import lax
from jax.experimental import pallas as pl
from jax.experimental.pallas import tpu as pltpu
from jax.sharding import PartitionSpec as P

HIGHER = 5
CROSS = 8
ROWS = 160
ROW_WEIGHT, ROW_BEFORE, ROW_DAMPING = 36, 37, 38
EDGES = (0, 8)
PIECE = 2048


def row_of(i, j):
    if i < 8 or j >= 8:
        base = 0 if i < 8 else 40
        a, b = i % 8, j % 8
        s = a - b
        return base + (s * 8 + b if s <= 4 else (8 - s) * 8 + a)
    return 80 + ((i - 8 - j) % 8) * 8 + j


def accumulate_kernel(count_hbm, design_hbm, unit_hbm, resid_hbm, weight_hbm, damping_hbm, keep_ref, send_ref, count_ref, design_ref, unit_ref, resid_ref, weight_ref, damping_ref, acc_ref, sems, small_sems):
    slots = design_ref.shape[1]
    units = acc_ref.shape[1]
    src = lax.axis_index("src")
    first_unit = lax.axis_index("tm") * units
    edges = [slots * e // 8 for e in EDGES]
    copies = [
        [
            pltpu.make_async_copy(hbm.at[:, pl.ds(lo, hi - lo)], ref.at[:, pl.ds(lo, hi - lo)], sems.at[c, n])
            for n, (hbm, ref) in enumerate(
                [(weight_hbm, weight_ref), (unit_hbm, unit_ref), (resid_hbm, resid_ref), (design_hbm, design_ref)]
            )
        ]
        for c, (lo, hi) in enumerate(zip(edges[:-1], edges[1:]))
    ]
    count_copy = pltpu.make_async_copy(count_hbm, count_ref, small_sems.at[0])
    damping_copy = pltpu.make_async_copy(damping_hbm, damping_ref, small_sems.at[1])
    count_copy.start()
    for group in copies:
        for copy in group:
            copy.start()
    damping_copy.start()
    count_copy.wait()
    count = count_ref[0]
    piece = min(PIECE, edges[1])
    own = damping_ref.shape[1]
    middle = units // 2
    inner = lax.broadcasted_iota(jnp.int32, (own, piece), 0)
    unit_rows = jnp.concatenate([inner + k * own for k in [*range(0, units // own, 2), *range(1, units // own, 2)]], axis=0)
    slot = lax.broadcasted_iota(jnp.int32, (1, piece), 1)
    total = jnp.zeros((2 * ROWS, units), jnp.float32)
    weight_sum = jnp.zeros((1, 128), jnp.float32)
    before_sum = jnp.zeros((1, 128), jnp.float32)
    for begin in range(0, slots, piece):
        if begin in edges:
            for copy in copies[edges.index(begin)]:
                copy.wait()
        at = pl.ds(begin, piece)
        rows = design_ref[:, at]
        resid = resid_ref[:, at]
        weight = jnp.where(slot + begin < count, weight_ref[:, at], 0.0)
        first, second = rows[:8], rows[8:]
        wfirst, wsecond = first * weight, second * weight
        groups = [wfirst * (pltpu.roll(first, 8 - s, 0) if s else first) for s in range(HIGHER)]
        turned = [pltpu.roll(second, 8 - s, 0) if s else second for s in range(CROSS)]
        groups += [wsecond * turned[s] for s in range(HIGHER)]
        groups += [wfirst * turned[s] for s in range(CROSS)]
        groups += [wfirst * resid, wsecond * resid]
        high, low = [], []
        for a, b in zip(groups[::2], groups[1::2]):
            both = jnp.concatenate([a, b], axis=0)
            top = both.astype(jnp.bfloat16)
            high.append(top)
            low.append((both - top.astype(jnp.float32)).astype(jnp.bfloat16))
        stacked = jnp.concatenate(high + low, axis=0)
        local = unit_ref[:, at] - first_unit
        one_hot = jnp.where(unit_rows == local, 1.0, 0.0).astype(jnp.bfloat16)
        total = total + lax.dot_general(stacked, one_hot, (((1,), (1,)), ((), ())), preferred_element_type=jnp.float32)
        before = weight * resid * resid
        for k in range(0, piece, 128):
            weight_sum = weight_sum + weight[:, k:k + 128]
            before_sum = before_sum + before[:, k:k + 128]
    acc_ref[...] = total[:ROWS] + total[ROWS:]
    acc_ref[ROW_WEIGHT:ROW_DAMPING + 1, :] = jnp.zeros((3, units), jnp.float32)
    acc_ref[ROW_WEIGHT:ROW_WEIGHT + 1, 0:128] = weight_sum
    acc_ref[ROW_BEFORE:ROW_BEFORE + 1, 0:128] = before_sum
    damping_copy.wait()
    padded = jnp.concatenate([damping_ref[...], jnp.zeros((1, units - own), jnp.float32)], axis=1)
    placed = pltpu.roll(jnp.broadcast_to(padded, (8, units)), (src // 2) * own + (src % 2) * middle, 1)
    acc_ref[ROW_DAMPING:ROW_DAMPING + 1, :] = placed[0:1]
    half = ROWS // 2
    plain = acc_ref[...]
    turned = pltpu.roll(plain, middle, 1)
    lanes = lax.broadcasted_iota(jnp.int32, (half, units), 1) < middle
    even = jnp.where(lanes, plain[:half], turned[half:])
    odd = jnp.where(lanes, turned[:half], plain[half:])
    is_even = src % 2 == 0
    keep_ref[...] = jnp.where(is_even, even, odd)
    send_ref[...] = jnp.where(is_even, odd, even)


def solve_kernel(mine_ref, solution_ref, stats_ref, full_ref, column_ref):
    units = mine_ref.shape[1]
    own = solution_ref.shape[0]
    src = lax.axis_index("src")
    half = ROWS // 2
    middle = units // 2
    full_ref[:half, :] = mine_ref[...]
    full_ref[half:, :] = pltpu.roll(mine_ref[...], middle, 1)
    column_ref[...] = jnp.zeros_like(column_ref)
    for j in range(16):
        for i in range(j, 16):
            r = row_of(i, j)
            column_ref[j * 24 + i:j * 24 + i + 1, :] = full_ref[r:r + 1, :]
        column_ref[j * 24 + 16:j * 24 + 17, :] = full_ref[144 + j:145 + j, :]
    damping = full_ref[ROW_DAMPING:ROW_DAMPING + 1, :]
    upper = [column_ref[j * 24:j * 24 + 8, :] for j in range(8)]
    lower = [column_ref[j * 24 + 8:j * 24 + 24, :] for j in range(16)]

    def entry(top, bottom, i):
        return top[i:i + 1] if i < 8 else bottom[i - 8:i - 7]

    inverse, forward = [], []
    for j in range(16):
        inv = lax.rsqrt(entry(upper[j] if j < 8 else None, lower[j], j) + damping)
        inverse.append(inv)
        if j < 8:
            upper[j] = upper[j] * inv
        lower[j] = lower[j] * inv
        forward.append(lower[j][8:9])
        for k in range(j + 1, 16):
            factor = entry(upper[j] if j < 8 else None, lower[j], k)
            lower[k] = lower[k] - lower[j] * factor
            if k < 8:
                upper[k] = upper[k] - upper[j] * factor
    sub = lax.broadcasted_iota(jnp.int32, (8, units), 0)
    low_x = jnp.zeros((8, units), jnp.float32)
    high_x = jnp.zeros((8, units), jnp.float32)
    for i in range(15, -1, -1):
        part = lower[i][:8] * high_x
        if i < 8:
            part = part + upper[i] * low_x
        x = (forward[i] - jnp.sum(part, axis=0, keepdims=True)) * inverse[i]
        if i < 8:
            low_x = jnp.where(sub == i, x, low_x)
        else:
            high_x = jnp.where(sub == i - 8, x, high_x)
    squares = damping * jnp.sum(low_x * low_x + high_x * high_x, axis=0, keepdims=True)
    for y in forward:
        squares = squares + y * y
    held = lax.broadcasted_iota(jnp.int32, (1, units), 1) < middle
    chi = jnp.sum(jnp.where(held, full_ref[ROW_BEFORE:ROW_BEFORE + 1, :] - squares, 0.0), axis=1, keepdims=True)
    weight = jnp.sum(jnp.where(held, full_ref[ROW_WEIGHT:ROW_WEIGHT + 1, :], 0.0), axis=1, keepdims=True)
    stats_ref[...] = jnp.where(lax.broadcasted_iota(jnp.int32, (8, 128), 0) == 0, chi, weight)
    shift = (units - (src // 2) * own) % units
    turned = pltpu.roll(jnp.concatenate([low_x, high_x], axis=0), shift, 1)
    solution_ref[...] = turned[:, :128].T[:own]


def quotient_kernel(*refs):
    parts = [ref[...] for ref in refs[:-1]]
    while len(parts) > 1:
        parts = [a + b for a, b in zip(parts[::2], parts[1::2])]
    refs[-1][...] = parts[0][0:1, 0:1] / parts[0][1:2, 0:1]


def in_vmem(x):
    return pltpu.with_memory_space_constraint(x, pltpu.VMEM)


def swap(x, axis, mask):
    size = lax.axis_size(axis)
    return lax.ppermute(x, axis, [(k, k ^ mask) for k in range(size)])


def masks_of(size):
    masks = []
    b = 1
    while (1 << b) < size:
        masks.append(1 << b)
        b += 1
    return masks


def on_device(design, unit_index, residual, weight, obs_count, damping):
    n_source = lax.axis_size("src")
    own_units = damping.shape[0]
    units = own_units * n_source
    slots = design.shape[1]
    half = ROWS // 2
    keep, send = pl.pallas_call(
        accumulate_kernel,
        in_specs=[pl.BlockSpec(memory_space=pltpu.HBM)] * 6,
        out_specs=[pl.BlockSpec(memory_space=pltpu.VMEM)] * 2,
        out_shape=[pltpu.VMEM((half, units), jnp.float32)] * 2,
        scratch_shapes=[
            pltpu.SMEM((1,), jnp.int32),
            pltpu.VMEM((16, slots), jnp.float32),
            pltpu.VMEM((1, slots), jnp.int32),
            pltpu.VMEM((1, slots), jnp.float32),
            pltpu.VMEM((1, slots), jnp.float32),
            pltpu.VMEM((1, own_units), jnp.float32),
            pltpu.VMEM((ROWS, units), jnp.float32),
            pltpu.SemaphoreType.DMA((len(EDGES) - 1, 4)),
            pltpu.SemaphoreType.DMA((2,)),
        ],
        name="accumulate",
    )(obs_count, design, unit_index.reshape(1, slots), residual.reshape(1, slots), weight.reshape(1, slots), damping.reshape(1, own_units))
    mine = keep + swap(send, "src", 1)
    for mask in masks_of(n_source):
        mine = mine + swap(mine, "src", mask)
    solution_own, stats = pl.pallas_call(
        solve_kernel,
        in_specs=[pl.BlockSpec(memory_space=pltpu.VMEM)],
        out_specs=[pl.BlockSpec(memory_space=pltpu.VMEM)] * 2,
        out_shape=[jax.ShapeDtypeStruct((own_units, 16), jnp.float32), pltpu.VMEM((8, 128), jnp.float32)],
        scratch_shapes=[pltpu.VMEM((ROWS, units), jnp.float32), pltpu.VMEM((16 * 24, units), jnp.float32)],
        name="solve",
    )(in_vmem(mine))
    n_time = lax.axis_size("tm")
    if n_time == 2:
        across = [(t * n_source + k, (t ^ 1) * n_source + (k ^ 1)) for t in range(2) for k in range(n_source)]
        parts = [stats, swap(stats, "src", 1), swap(stats, "tm", 1), lax.ppermute(stats, ("tm", "src"), across)]
    else:
        stats = stats + swap(stats, "src", 1)
        mask = 1
        while 2 * mask < n_time:
            stats = stats + swap(stats, "tm", mask)
            mask *= 2
        parts = [stats, swap(stats, "tm", mask)] if n_time > 1 else [stats]
    misfit = pl.pallas_call(
        quotient_kernel,
        in_specs=[pl.BlockSpec(memory_space=pltpu.VMEM)] * len(parts),
        out_shape=jax.ShapeDtypeStruct((1, 1), jnp.float32),
        name="quotient",
    )(*[in_vmem(part) for part in parts])
    return (solution_own.T, misfit.reshape(()))


def solution(mesh):
    placed = (
        P(None, ("tm", "src")),
        P(("tm", "src")),
        P(("tm", "src")),
        P(("tm", "src")),
        P(("tm", "src")),
        P(("tm", "src")),
    )
    return jax.shard_map(
        on_device,
        mesh=mesh,
        in_specs=placed,
        out_specs=(P(None, ("tm", "src")), P()),
        check_vma=False,
    )
```
